32 devices in a mesh: tok: 8 (over z, core), vocab: 4 (over y, x).
Axes of the slice: x: 2, y: 2, z: 4, core: 2. Of those that a mesh axis runs over, the one named last changes fastest.
Arguments:
- latent_vectors: float32 [768, 3584], P('tok'), may hold values from -400 to 400
- unembedding_matrix: float32 [3584, 152064], P(None, ('tok', 'vocab')), may hold values from -0.09375 to 0.09375
- drawn_symbols: int32 [768], P('tok'), may hold values from 0 to 152063
- piece_extents: int32 [8, 4], P('tok'), may hold values from 1 to 48, 96 in all within a row
- piece_episode_lookup: int32 [8, 4], P('tok'), may hold values from 0 to 1023
- episode_heats: float32 [1024], replicated, may hold values from 0.6 to 1.5
Outputs:
- seg_logprob: float32 [32], P('tok')
The draws below stay inside these ranges and needn't reach their ends.
Inputs may be any that keep to these rules, and one draw needn't show every extreme that they name: `piece_extents`: each row of lengths sums to 96.
All inputs are finite; a program needn't handle non-finite values.
Results may differ from the reference program's by a relative error of at most 0.0003.
Values sent between devices are 32-bit elements; how exact they have to be, the bound alone decides.
No kernel may reach another device: no remote copies, remote signals or barrier semaphores. Data moves between devices by JAX's collectives and lax.ppermute only.
A program may use at most 128 MiB of HBM per device.

```python
import math
import jax
import jax.numpy as jnp
import numpy as np
from jax import lax

H = 3584
V = 152064
TOK_DEV = 96
SEG_DEV = 4
EPISODE_NUMBER = 1024
TOKENS = 768
SEGMENTS = 32
N_TOK = 8
N_VOCAB = 4


def draw_latent_vectors(key, part):
    values = jax.random.normal(key, (TOKENS, H), jnp.float32) * 3.0
    return jnp.clip(values, -400.0, 400.0).astype(jnp.float32)


def place_ends(result, own_key, low, top_value):
    index_at = [jax.random.randint(jax.random.fold_in(own_key, axis), (), 0, length) for axis, length in enumerate(result.shape)]
    widest = result.shape.index(max(result.shape))
    beside = index_at[:widest] + [(index_at[widest] + 1) % result.shape[widest]] + index_at[widest + 1:]
    return result.at[tuple(index_at)].set(low).at[tuple(beside)].set(top_value)


def steps_of(key, dims, shards, least, top_value):
    factor_of, own = 1.0, jax.random.fold_in(key, 6)
    for dim, parts in shards:
        draws = jnp.exp(jax.random.uniform(jax.random.fold_in(own, dim), (parts,), jnp.float32, least / len(shards), top_value / len(shards)))
        factor_of = factor_of * jnp.repeat(draws, dims[dim] // parts).reshape([-1 if axis == dim else 1 for axis in range(len(dims))])
    return factor_of


def ranked_wide(own_key, dims, number_of, lean):
    weights = [min(1 << octave, number_of + 1 - (1 << octave)) * (1 << 20) // math.isqrt((1 << octave) ** lean) + 1 for octave in range((number_of + 1).bit_length()) if 1 << octave <= number_of]
    scale = 1 + sum(weights) // (1 << 30)
    table = np.cumsum(np.array([max(1, weight // scale) for weight in weights]))
    ticket = jax.random.randint(jax.random.fold_in(own_key, 1), dims, 0, int(table[len(weights) - 1]))
    start = jnp.left_shift(1, jnp.searchsorted(jnp.asarray(table, jnp.int32), ticket, side="right").astype(jnp.int32))
    grade = start - 1 + jax.random.randint(jax.random.fold_in(own_key, 4), dims, 0, 1 << 30) % jnp.minimum(start, number_of + 1 - start)
    return jax.random.permutation(jax.random.fold_in(own_key, 2), number_of)[grade].astype(jnp.int32)


def split_up(amount, total, bound, slope):
    weights = [(1 << 20) // math.isqrt(grade ** slope) + 1 for grade in range(2, amount + 1)]
    spare, given = total - bound - (amount - 1), [1] * (amount - 1)
    while spare > 0:
        free = [i for i in range(amount - 1) if given[i] < bound]
        mass, remaining = sum([weights[i] for i in free]), spare
        for i in free:
            addition = min(bound - given[i], max(1, remaining * weights[i] // mass), spare)
            given[i] = given[i] + addition
            spare = spare - addition
    return np.array([bound] + given)


def uneven(rng, count, total, limit, lean):
    if count == 2:
        one = jax.random.randint(rng, (), max(1, total - limit), min(limit, total - 1) + 1)
        return jnp.stack([one, total - one])
    sizes = jnp.asarray(split_up(count, total, limit, lean), jnp.int32)
    twos = (count - 1) // 2
    source_of, sink = sizes[1:1 + 2 * twos:2], sizes[2:2 + 2 * twos:2]
    room = jnp.minimum(source_of - 1, limit - sink)
    moved = jax.random.randint(jax.random.fold_in(rng, 1), (twos,), 0, 1 << 20) % (room + 1)
    sizes = sizes.at[1:1 + 2 * twos:2].set(source_of - moved).at[2:2 + 2 * twos:2].set(sink + moved)
    return sizes[jax.random.permutation(jax.random.fold_in(rng, 2), count)]


def centred(own_key, extent, scale, reach, cuts=(), held_as=jnp.bfloat16):
    result = jax.random.normal(own_key, extent, jnp.float32) * scale
    if len(cuts) > 0:
        result = steps_of(own_key, extent, cuts, -0.22, 0.18) * result
    return jnp.clip(result, min=-reach, max=reach).astype(held_as)


def setup_inputs(seed: int = 0) -> dict:
    seeds = jax.random.split(jax.random.key(seed), 7)
    return {
        "latent_vectors": draw_latent_vectors(jax.random.fold_in(seeds[6], 71), 0),
        "unembedding_matrix": centred(seeds[1], (H, V), H ** -0.5, 0.09375, ((1, 32),), jnp.float32),
        "drawn_symbols": place_ends(ranked_wide(seeds[2], (TOKENS,), V, 2), jax.random.fold_in(seeds[2], 3), 0, V - 1).astype(jnp.int32),
        "piece_extents": jax.vmap(lambda own: uneven(own, SEG_DEV, TOK_DEV, TOK_DEV // 2, 2))(jax.random.split(seeds[3], N_TOK)).reshape((N_TOK, SEG_DEV)).astype(jnp.int32),
        "piece_episode_lookup": place_ends(jax.random.randint(seeds[4], (N_TOK, SEG_DEV), 0, EPISODE_NUMBER), jax.random.fold_in(seeds[4], 1), 0, EPISODE_NUMBER - 1).astype(jnp.int32),
        "episode_heats": jnp.clip(jnp.exp(jax.random.uniform(seeds[5], (EPISODE_NUMBER,), jnp.float32, math.log(0.6), math.log(1.5))), 0.6, 1.5),
    }


def line_heat_divisor(piece_extents, piece_episode_lookup, episode_heats):
    ends = jnp.cumsum(piece_extents, axis=1)
    starts = ends - piece_extents
    position = jnp.arange(TOK_DEV, dtype=jnp.int32)
    piece_episode = ((position[None, None, :] >= starts[:, :, None]) & (position[None, None, :] < ends[:, :, None])).astype(jnp.float32)
    chosen_symbol = (piece_episode_lookup[:, :, None] == jnp.arange(EPISODE_NUMBER, dtype=jnp.int32)[None, None, :]).astype(jnp.float32)
    piece_reciprocal_heat = jnp.einsum("rto,o->rt", chosen_symbol, 1.0 / episode_heats, precision=lax.Precision.HIGHEST)
    symbol_reciprocal_heat = jnp.einsum("sgp,sg->sp", piece_episode, piece_reciprocal_heat, precision=lax.Precision.HIGHEST)
    return piece_episode, symbol_reciprocal_heat.reshape(TOKENS)


def reference(latent_vectors, unembedding_matrix, drawn_symbols, piece_extents, piece_episode_lookup, episode_heats):
    piece_episode, symbol_reciprocal_heat = line_heat_divisor(piece_extents, piece_episode_lookup, episode_heats)
    width = V // (N_TOK * N_VOCAB)

    def block_step(carry, index):
        start = (index * width).astype(jnp.int32)
        columns = lax.dynamic_slice_in_dim(unembedding_matrix, start, width, 1)
        logits = jnp.dot(latent_vectors, columns, preferred_element_type=jnp.float32, precision=lax.Precision.HIGHEST) * symbol_reciprocal_heat[:, None]
        block_top = jnp.max(logits, axis=1)
        block_total = jnp.sum(jnp.exp(logits - block_top[:, None]), axis=1)
        ids = start + jnp.arange(width, dtype=jnp.int32)
        block_picked = jnp.sum(jnp.where(drawn_symbols[:, None] == ids[None, :], logits, 0.0), axis=1)
        return carry, (block_top, block_total, block_picked)

    unused, (tops, totals, pickeds) = lax.scan(block_step, jnp.zeros((), jnp.float32), jnp.arange(N_TOK * N_VOCAB, dtype=jnp.int32))
    top = jnp.max(tops, axis=0)
    total = jnp.sum(totals * jnp.exp(tops - top[None, :]), axis=0)
    picked = jnp.sum(pickeds, axis=0)
    logprob = picked - top - jnp.log(total)
    sums = jnp.einsum("sgp,sp->sg", piece_episode, logprob.reshape(N_TOK, TOK_DEV), precision=lax.Precision.HIGHEST)
    return (sums / piece_extents.astype(jnp.float32)).reshape(SEGMENTS)
```

```python
import functools

import jax
import jax.numpy as jnp
from jax import lax
from jax.experimental import pallas as pl
from jax.experimental.pallas import tpu as pltpu
from jax.sharding import PartitionSpec as P


LANES = 128
NT = (((1,), (1,)), ((), ()))


def chunk_widths(total):
    units = total // LANES
    parts = [max(1, units * w // 28) for w in (3, 8)]
    parts.append(units - sum(parts))
    return [p * LANES for p in parts if p > 0]


def tile_of(width, limit=528):
    best = width
    for t in range(16, limit + 1, 16):
        if width % t == 0:
            best = t
    return best if best <= limit else width


def split(v):
    hi = v.astype(jnp.bfloat16)
    return hi, (v - hi.astype(jnp.float32)).astype(jnp.bfloat16)


def gemm_kernel(first, last, half, k, tile, *refs):
    refs = list(refs)
    base_ref = refs.pop(0) if last else None
    own_ref, sib_ref, w_ref = refs.pop(0), refs.pop(0), refs.pop(0)
    acc_ref = None if first else refs.pop(0)
    out_ref = refs.pop(0)
    xh_ref, xl_ref = refs.pop(0), refs.pop(0)
    i = pl.program_id(0)
    tokens = 2 * half

    @pl.when(i == 0)
    def _():
        for p, ref in enumerate((own_ref, sib_ref)):
            hi, lo = split(ref[:, :k])
            xh_ref[p * half:(p + 1) * half, :] = hi
            xl_ref[p * half:(p + 1) * half, :] = lo

    wh, wl = split(w_ref[...])
    xh, xl = xh_ref[...], xl_ref[...]
    dot = functools.partial(
        lax.dot_general, dimension_numbers=NT, preferred_element_type=jnp.float32
    )
    part = dot(wh, xh) + dot(wh, xl) + dot(wl, xh)
    if not first:
        part = part + acc_ref[...]
    if not last:
        out_ref[...] = part
        return
    row_ref = refs.pop(0)

    @pl.when(i == 0)
    def _():
        for p, ref in enumerate((own_ref, sib_ref)):
            row_ref[:, p * half:(p + 1) * half] = ref[:, k:k + LANES].T[:8]
        out_ref[...] = jnp.concatenate(
            [jnp.full((1, tokens), -jnp.inf, jnp.float32), jnp.zeros((7, tokens), jnp.float32)]
        )

    logits = part * row_ref[0:1, :]
    target = row_ref[1:2, :].astype(jnp.int32)
    ids = base_ref[0] + i * tile + lax.broadcasted_iota(jnp.int32, (tile, tokens), 0)
    old = out_ref[0:1, :]
    top = jnp.maximum(old, jnp.max(logits, axis=0, keepdims=True))
    total = out_ref[1:2, :] * jnp.exp(old - top) + jnp.sum(
        jnp.exp(logits - top), axis=0, keepdims=True
    )
    picked = out_ref[2:3, :] + jnp.sum(
        jnp.where(ids == target, logits, 0.0), axis=0, keepdims=True
    )
    out_ref[0:1, :] = top
    out_ref[1:2, :] = total
    out_ref[2:3, :] = picked


def gemm(own, sib, w_t, acc, base, offset, k, last):
    width = w_t.shape[0]
    half = own.shape[0]
    tokens = 2 * half
    tile = tile_of(width)
    first = acc is None
    vm = pl.BlockSpec(memory_space=pltpu.VMEM)
    block = pl.BlockSpec((tile, tokens), lambda i: (i, 0))
    specs = [pl.BlockSpec(memory_space=pltpu.SMEM)] if last else []
    specs += [vm, vm, pl.BlockSpec((pl.Element(tile), pl.Element(k)), lambda i: (i * tile if tile < width else 0, offset))]
    args = ([base] if last else []) + [own, sib, w_t]
    alias = {}
    if not first:
        specs.append(block)
        args.append(acc)
        if not last:
            alias = {len(args) - 1: 0}
    scratch = [pltpu.VMEM((tokens, k), jnp.bfloat16)] * 2
    if last:
        scratch.append(pltpu.VMEM((8, tokens), jnp.float32))
        out_spec, out_shape = vm, (8, tokens)
    else:
        out_spec, out_shape = block, (width, tokens)
    return pl.pallas_call(
        functools.partial(gemm_kernel, first, last, half, k, tile),
        grid=(width // tile,),
        in_specs=specs,
        out_specs=out_spec,
        out_shape=jax.ShapeDtypeStruct(out_shape, jnp.float32),
        scratch_shapes=scratch,
        input_output_aliases=alias,
        compiler_params=pltpu.CompilerParams(
            dimension_semantics=("arbitrary",), vmem_limit_bytes=60 * 1024 * 1024
        ),
        cost_estimate=pl.CostEstimate(
            flops=6 * tokens * width * k, bytes_accessed=4 * width * (k + 2 * tokens), transcendentals=0
        ),
        name="gemm_last" if last else "gemm",
    )(*args)


def aug_kernel(extent_ref, lookup_ref, heat_ref, symbol_ref, out_ref):
    rows = out_ref.shape[0]
    row = lax.broadcasted_iota(jnp.int32, (rows, LANES), 0)
    lane = lax.broadcasted_iota(jnp.int32, (rows, LANES), 1)
    heat = jnp.ones((rows, LANES), jnp.float32)
    start = jnp.int32(0)
    for s in range(extent_ref.shape[1]):
        end = start + extent_ref[0, s]
        heat = jnp.where((row >= start) & (row < end), heat_ref[lookup_ref[0, s]], heat)
        start = end
    out_ref[...] = jnp.where(lane == 1, symbol_ref[...].astype(jnp.float32), 1.0 / heat)


def tail_kernel(extent_ref, stat_ref, out_ref):
    tops = stat_ref[:, :LANES]
    totals = stat_ref[:, LANES:2 * LANES]
    picks = stat_ref[:, 2 * LANES:]
    top = jnp.max(tops, axis=0, keepdims=True)
    total = jnp.sum(totals * jnp.exp(tops - top), axis=0, keepdims=True)
    picked = jnp.sum(picks, axis=0, keepdims=True)
    logprob = picked - top - jnp.log(total)
    lane = lax.broadcasted_iota(jnp.int32, (1, LANES), 1)
    start = jnp.int32(0)
    result = jnp.zeros((1, LANES), jnp.float32)
    for s in range(extent_ref.shape[1]):
        size = extent_ref[0, s]
        end = start + size
        inside = (lane >= start) & (lane < end)
        mean = jnp.sum(jnp.where(inside, logprob, 0.0), axis=1, keepdims=True) / size.astype(
            jnp.float32
        )
        result = jnp.where(lane == s, mean, result)
        start = end
    out_ref[...] = result


def turn(a, index, axis):
    n = a.shape[axis]
    return lax.dynamic_slice_in_dim(
        jnp.concatenate([a, a], axis=axis), lax.rem(n - index, n), n, axis
    )


def on_device(cores, latent, w, symbols, extents, lookup, heats):
    rows, width_k = latent.shape
    width = w.shape[1]
    n_tok, n_vocab = lax.axis_size("tok"), lax.axis_size("vocab")
    nz = n_tok // cores
    t, v = lax.axis_index("tok"), lax.axis_index("vocab")
    z, c = t // cores, lax.rem(t, cores)
    part = rows // n_vocab
    w_t = w.T
    sm = pl.BlockSpec(memory_space=pltpu.SMEM)
    vm = pl.BlockSpec(memory_space=pltpu.VMEM)

    aug = pl.pallas_call(
        aug_kernel,
        in_specs=[sm, sm, sm, vm],
        out_specs=vm,
        out_shape=jax.ShapeDtypeStruct((rows, LANES), jnp.float32),
        name="aug",
    )(extents, lookup, heats, symbols[:, None])

    widths = chunk_widths(width_k)
    blocks, start = [], 0
    for j, k in enumerate(widths):
        piece = latent[:, start:start + k]
        if j == len(widths) - 1:
            piece = jnp.concatenate([piece, aug], axis=1)
        blocks.append((start, k, piece))
        start += k

    from_z = lambda a, s: lax.ppermute(
        a, "tok", [(((q // cores + s) % nz) * cores + q % cores, q) for q in range(n_tok)]
    )
    from_v = lambda a, u: lax.ppermute(
        a, "vocab", [((q + u) % n_vocab, q) for q in range(n_vocab)]
    )
    sibling = lambda a: lax.ppermute(a, "tok", [(q ^ 1, q) for q in range(n_tok)])

    acc = None
    base = ((t * n_vocab + v) * width).astype(jnp.int32).reshape(1)
    for j, (start, k, piece) in enumerate(blocks):
        mine = lax.dynamic_slice_in_dim(piece, v * part, part, 0)
        far = []
        for s in range(1, nz):
            far.append(from_z(mine, s))
        far = jnp.concatenate(far)
        own = [piece, far]
        for u in range(1, n_vocab):
            own.append(from_v(far, u))
        own = jnp.concatenate(own)
        sib = sibling(own)
        acc = gemm(own, sib, w_t, acc, base, start, k, j == len(blocks) - 1)

    stats = acc[:3].reshape(3, cores, nz * rows)
    near = stats[:, :, :rows].reshape(3, cores, 1, rows)
    far = stats[:, :, rows:].reshape(3, cores, n_vocab, nz - 1, part)
    far = turn(far, v, 2).transpose(0, 1, 3, 2, 4).reshape(3, cores, nz - 1, rows)
    full = jnp.concatenate([near, far], axis=2)
    full = turn(turn(full, z, 2), c, 1).transpose(2, 1, 0, 3).reshape(n_tok, 3, rows)
    full = jnp.pad(full, ((0, 0), (0, 0), (0, LANES - rows))).reshape(n_tok, 1, 3 * LANES)
    full = jnp.broadcast_to(full, (n_tok, n_vocab, 3 * LANES)).reshape(-1, 3 * LANES)
    stats = lax.all_to_all(full, ("tok", "vocab"), 0, 0, tiled=True)

    out = pl.pallas_call(
        tail_kernel,
        in_specs=[sm, vm],
        out_specs=vm,
        out_shape=jax.ShapeDtypeStruct((1, LANES), jnp.float32),
        name="tail",
    )(extents, stats)
    return out[0, :extents.shape[1]]


def body(cores, *args):
    return on_device(cores, *args)


def solution(mesh):
    cores = 2
    return jax.shard_map(
        functools.partial(body, cores),
        mesh=mesh,
        in_specs=(
            P("tok", None),
            P(None, ("tok", "vocab")),
            P("tok"),
            P("tok", None),
            P("tok", None),
            P(),
        ),
        out_specs=P("tok"),
        check_vma=False,
    )
```
